32 devices in a mesh: morton: 8 (over z, x), grp: 4 (over y, core).
Axes of the slice: x: 2, y: 2, z: 4, core: 2. Of those that a mesh axis runs over, the one named last changes fastest.
Arguments:
- multipoles: float32 [2048, 152], P(('morton', 'grp')), may hold values from -6 to 6
- chebyshev: float32 [2048, 560], P(('morton', 'grp')), may hold values from -6 to 6
- ghost_rows: int32 [64, 64], P('morton'), may hold values from 0 to 255
- far_src: int32 [2048, 189], P(('morton', 'grp')), may hold values from 0 to 767
- far_kind: int32 [2048, 189], P(('morton', 'grp')), may hold values from 0 to 15
- far_count: int32 [2048], P(('morton', 'grp')), may hold values from 1 to 189
- near_src: int32 [2048, 27], P(('morton', 'grp')), may hold values from 0 to 191, as said below
- near_kind: int32 [2048, 27], P(('morton', 'grp')), may hold values from 0 to 3
- far_ops: float32 [16, 152, 152], replicated, may hold values from -0.046875 to 0.046875
- near_ops: float32 [4, 560, 560], replicated, may hold values from -0.046875 to 0.046875
- local_to_target: float32 [152, 560], replicated, may hold values from -0.5 to 0.5
Outputs:
- potential: float32 [2048, 560], P(('morton', 'grp'))
The draws below stay inside these ranges and needn't reach their ends.
Inputs may be any that keep to these rules, and one draw needn't show every extreme that they name: Entries below 256 name a box of the target's own range; the others name ghost number far_src - 256 of its far ghost list. Entries below 64 name a box of the target's own device; the others name ghost number near_src - 64 of its range's near ghost list.
All inputs are finite; a program needn't handle non-finite values.
Results may differ from the reference program's by a relative error of at most 0.0003.
Values sent between devices are 32-bit elements; how exact they have to be, the bound alone decides.
No kernel may reach another device: no remote copies, remote signals or barrier semaphores. Data moves between devices by JAX's collectives and lax.ppermute only.
A program may use at most 64 MiB of HBM per device.

```python
import jax
import jax.numpy as jnp
from jax import lax

P_SIZE = 152
Q = 560
FAR = 189
NEAR = 27
FCLS = 16
NCLS = 4
CAP = 64
NCAP = 16
BOX_DEV = 64
RANGE = 256
BOXES = 2048
FTABLE = 768
NTABLE = 192
N_MORTON = 8
N_GRP = 4


def draw_near_src(key, part):
    pick_key = jax.random.fold_in(key, 11)
    own_key = jax.random.fold_in(key, 12)
    ghost_key = jax.random.fold_in(key, 13)
    shape = (BOXES, NEAR)
    selector = jax.random.randint(pick_key, shape, 0, 10)
    own_entry = jax.random.randint(own_key, shape, 0, BOX_DEV)
    ghost_entry = jax.random.randint(ghost_key, shape, BOX_DEV, NTABLE)
    return jnp.where(selector < 7, own_entry, ghost_entry).astype(jnp.int32)


def with_ends(values, stream_key, low, largest):
    dims = values.shape
    place = [jax.random.randint(jax.random.fold_in(stream_key, axis), (), 0, dims[axis]) for axis in range(len(dims))]
    values = values.at[tuple(place)].set(low)
    longest = dims.index(max(dims))
    place[longest] = (place[longest] + 1) % dims[longest]
    return values.at[tuple(place)].set(largest)


def shard_levels(key, shape, cuts, least, largest):
    def one(dim, shards_of):
        draws = jax.random.uniform(jax.random.fold_in(jax.random.fold_in(key, 6), dim), (shards_of,), jnp.float32, least / len(cuts), largest / len(cuts))
        return jnp.repeat(jnp.exp(draws), shape[dim] // shards_of).reshape((-1,) + (1,) * (len(shape) - dim - 1))

    level = one(*cuts[0])
    for cut in cuts[1:]:
        level = level * one(*cut)
    return level


def noise(key, extent, spread, most, shards=(), kind=jnp.bfloat16):
    values = spread * jax.random.normal(key, extent, jnp.float32)
    if shards:
        values = values * shard_levels(key, extent, shards, -0.22, 0.18)
    return jnp.clip(values, -most, most).astype(kind)


def setup_inputs(seed: int = 0) -> dict:
    keys = jax.random.split(jax.random.key(seed), 12)
    return {
        "multipoles": noise(keys[0], (BOXES, P_SIZE), 1.0, 6.0, ((0, 32),), jnp.float32),
        "chebyshev": noise(keys[1], (BOXES, Q), 1.0, 6.0, ((0, 32),), jnp.float32),
        "ghost_rows": with_ends(jax.random.randint(keys[2], (N_MORTON * N_MORTON, CAP), 0, RANGE), jax.random.fold_in(keys[2], 1), 0, RANGE - 1).astype(jnp.int32),
        "far_src": with_ends(jax.random.randint(keys[3], (BOXES, FAR), 0, FTABLE), jax.random.fold_in(keys[3], 1), 0, FTABLE - 1).astype(jnp.int32),
        "far_kind": with_ends(jax.random.randint(keys[4], (BOXES, FAR), 0, FCLS), jax.random.fold_in(keys[4], 1), 0, FCLS - 1).astype(jnp.int32),
        "far_count": with_ends(jax.random.randint(keys[5], (BOXES,), 1, FAR + 1), jax.random.fold_in(keys[5], 1), 1, FAR).astype(jnp.int32),
        "near_src": draw_near_src(jax.random.fold_in(keys[11], 71), 0),
        "near_kind": with_ends(jax.random.randint(keys[7], (BOXES, NEAR), 0, NCLS), jax.random.fold_in(keys[7], 1), 0, NCLS - 1).astype(jnp.int32),
        "far_ops": noise(keys[8], (FCLS, P_SIZE, P_SIZE), (P_SIZE * FAR // 2) ** -0.5, 0.046875, (), jnp.float32),
        "near_ops": noise(keys[9], (NCLS, Q, Q), (Q * NEAR) ** -0.5, 0.046875, (), jnp.float32),
        "local_to_target": noise(keys[10], (P_SIZE, Q), P_SIZE ** -0.5, 0.5, (), jnp.float32),
    }


def class_sum(lookup, indices, weight, class_ids, classes):
    targets, slot_count = indices.shape
    picked = lookup[indices] * weight[:, :, None]
    segment = (jnp.arange(targets, dtype=jnp.int32)[:, None] * classes + class_ids).reshape(-1)
    summed = jax.ops.segment_sum(picked.reshape(targets * slot_count, lookup.shape[1]), segment, num_segments=targets * classes)
    return summed.reshape(targets, classes, lookup.shape[1])


def evaluate(far_table, near_table, far_src, far_kind, far_count, near_src, near_kind, far_ops, near_ops, local_to_target):
    active = (jnp.arange(far_src.shape[1], dtype=jnp.int32)[None, :] < far_count[:, None]).astype(far_table.dtype)
    far_sum = class_sum(far_table, far_src, active, far_kind, far_ops.shape[0])
    local_field = jnp.einsum("tkp,kpq->tq", far_sum, far_ops, precision=lax.Precision.HIGHEST)
    unit_weight = jnp.ones(near_src.shape, near_table.dtype)
    near_sum = class_sum(near_table, near_src, unit_weight, near_kind, near_ops.shape[0])
    near_field = jnp.einsum("tkc,kcd->td", near_sum, near_ops, precision=lax.Precision.HIGHEST)
    return jnp.dot(local_field, local_to_target, precision=lax.Precision.HIGHEST) + near_field


def reference(multipoles, chebyshev, ghost_rows, far_src, far_kind, far_count, near_src, near_kind, far_ops, near_ops, local_to_target):
    starts = jnp.arange(N_MORTON, dtype=jnp.int32)[:, None] * RANGE
    ghost_table = ghost_rows.reshape(N_MORTON, N_MORTON, CAP)

    def device(position):
        anchor = (position // N_GRP).astype(jnp.int32)
        far_ids = (starts + ghost_table[:, anchor, :]).reshape(-1).astype(jnp.int32)
        near_ids = (starts + ghost_table[:, anchor, :NCAP]).reshape(-1).astype(jnp.int32)
        range_multi = lax.dynamic_slice_in_dim(multipoles, (anchor * RANGE).astype(jnp.int32), RANGE, 0)
        far_table = jnp.concatenate([range_multi, multipoles[far_ids]], axis=0)
        first = (position * BOX_DEV).astype(jnp.int32)
        own_cheb = lax.dynamic_slice_in_dim(chebyshev, first, BOX_DEV, 0)
        near_table = jnp.concatenate([own_cheb, chebyshev[near_ids]], axis=0)

        def mine(array):
            return lax.dynamic_slice_in_dim(array, first, BOX_DEV, 0)

        return evaluate(far_table, near_table, mine(far_src), mine(far_kind), mine(far_count), mine(near_src), mine(near_kind), far_ops, near_ops, local_to_target)

    result = lax.map(device, jnp.arange(N_MORTON * N_GRP, dtype=jnp.int32))
    return result.reshape(BOXES, Q)
```

```python
import functools

import jax
import jax.numpy as jnp
from jax import lax
from jax.experimental import pallas as pl
from jax.experimental.pallas import tpu as pltpu
from jax.sharding import PartitionSpec as P

NCAP = 16
LANES = 128
F32 = jnp.float32
BF16 = jnp.bfloat16


def cdiv(a, b):
    return -(-a // b)


def split(x):
    hi = x.astype(BF16)
    return hi, (x - hi.astype(F32)).astype(BF16)


def mm(a, b):
    return lax.dot_general(a, b, (((1,), (0,)), ((), ())), preferred_element_type=F32)


def counts_kernel(dims, cnt_ref, fsrc_ref, fkind_ref, nsrc_ref, nkind_ref, fops_ref, nops_ref, l2t_ref,
                  wf_ref, wn_ref, fh_ref, fl_ref, nh_ref, nl_ref, lh_ref, ll_ref, c_ref, lo_ref):
    targets, far, near, fcls, ncls, fhi, nhi, rows, slots, near_at, nrows = dims
    group = 4
    fsrc = fsrc_ref[...]
    nsrc = nsrc_ref[...]
    c_ref[...] = jnp.full(c_ref.shape, -1, jnp.int32)
    lo_ref[...] = jnp.zeros(lo_ref.shape, jnp.int32)
    c_ref[:, :far] = (fsrc >> 7) * fcls + fkind_ref[...]
    lo_ref[:, :far] = fsrc & (LANES - 1)
    c_ref[:, near_at:near_at + near] = fhi * fcls + (nsrc >> 7) * ncls + nkind_ref[...]
    lo_ref[:, near_at:near_at + near] = nsrc & (LANES - 1)
    lane = lax.broadcasted_iota(jnp.int32, (1, slots), 1)
    row_id = lax.broadcasted_iota(jnp.int32, (rows, slots), 0)
    lo_id = lax.broadcasted_iota(jnp.int32, (LANES, slots), 0)

    def body(step, carry):
        for i in range(group):
            t = step * group + i
            live = (lane < cnt_ref[t]) | (lane >= near_at)
            c_row = jnp.where(live, c_ref[pl.ds(t, 1), :], -1)
            one_c = jnp.where(row_id == c_row, 1.0, 0.0).astype(BF16)
            one_lo = jnp.where(lo_id == lo_ref[pl.ds(t, 1), :], 1.0, 0.0).astype(BF16)
            w = lax.dot_general(one_c, one_lo, (((1,), (1,)), ((), ())), preferred_element_type=F32)
            at = pl.multiple_of(t * fcls, fcls)
            for h in range(fhi):
                wf_ref[pl.ds(at, fcls), h * LANES:(h + 1) * LANES] = w[h * fcls:(h + 1) * fcls].astype(BF16)
            wn_ref[pl.ds(pl.multiple_of(t * nrows, nrows), nrows), :] = w[fhi * fcls:fhi * fcls + nrows]
        return carry

    lax.fori_loop(0, targets // group, body, 0)
    for k in range(fcls):
        fh_ref[k], fl_ref[k] = split(fops_ref[k])
    for k in range(ncls):
        nh_ref[k], nl_ref[k] = split(nops_ref[k])
    lh_ref[...], ll_ref[...] = split(l2t_ref[...])


def dot3(x, wh, wl):
    xh, xl = split(x)
    both = mm(jnp.concatenate([xh, xl], axis=0), wh)
    n = x.shape[0]
    return both[:n] + both[n:] + mm(xh, wl)


def field_kernel(dims, wf_ref, wn_ref, fh_ref, fl_ref, nh_ref, nl_ref, lh_ref, ll_ref,
                 rm_ref, gm_ref, oc_ref, gc_ref, out_ref, fs_ref):
    targets, far, near, fcls, ncls, fhi, nhi, rows, slots, near_at, nrows = dims
    own = rm_ref.shape[0]
    ghosts = gm_ref.shape[0]
    rh, rl = split(rm_ref[...])
    gh, gl = split(gm_ref[...])
    wr = wf_ref[:, :own]
    wg = wf_ref[:, own:own + ghosts]
    width = rm_ref.shape[1]
    far_sum = mm(wr, rh) + mm(wr, rl) + mm(wg, gh) + mm(wg, gl)
    cuts = [(at, min(at + LANES, width)) for at in range(0, width, LANES)]
    for i, (first, last) in enumerate(cuts):
        fs_ref[i, :, :last - first] = far_sum[:, first:last]
    local = jnp.zeros((targets, width), F32)
    for k in range(fcls):
        x = jnp.concatenate(
            [fs_ref[i, pl.ds(k, targets, stride=fcls), :][:, :last - first] for i, (first, last) in enumerate(cuts)],
            axis=1)
        local += dot3(x, fh_ref[k], fl_ref[k])
    acc = dot3(local, lh_ref[...], ll_ref[...])
    table = jnp.concatenate([oc_ref[...], gc_ref[...]], axis=0)
    th, tl = split(table)
    length = table.shape[0]
    sums = jnp.zeros((ncls * targets, table.shape[1]), F32)
    for h in range(nhi):
        first, last = h * LANES, min((h + 1) * LANES, length)
        w = jnp.concatenate(
            [wn_ref[pl.ds(h * ncls + k, targets, stride=nrows), :] for k in range(ncls)], axis=0
        ).astype(BF16)[:, :last - first]
        sums += mm(w, th[first:last]) + mm(w, tl[first:last])
    for k in range(ncls):
        acc += dot3(sums[k * targets:(k + 1) * targets], nh_ref[k], nl_ref[k])
    out_ref[...] = acc


def shards(multipoles, chebyshev, ghost_rows, far_src, far_kind, far_count, near_src, near_kind,
           far_ops, near_ops, local_to_target):
    targets, width_p = multipoles.shape
    width_q = chebyshev.shape[1]
    fcls, ncls = far_ops.shape[0], near_ops.shape[0]
    far, near = far_src.shape[1], near_src.shape[1]
    range_multi = lax.all_gather(multipoles, "grp", axis=0, tiled=True)
    range_cheb = lax.all_gather(chebyshev, "grp", axis=0, tiled=True)
    near_rows = ghost_rows[:, :NCAP]
    ghost_multi = lax.all_to_all(range_multi[ghost_rows], "morton", split_axis=0, concat_axis=0, tiled=True)
    ghost_cheb = lax.all_to_all(range_cheb[near_rows], "morton", split_axis=0, concat_axis=0, tiled=True)
    ghost_multi = ghost_multi.reshape(-1, width_p)
    ghost_cheb = ghost_cheb.reshape(-1, width_q)

    ftable = range_multi.shape[0] + ghost_multi.shape[0]
    ntable = targets + ghost_cheb.shape[0]
    fhi, nhi = cdiv(ftable, LANES), cdiv(ntable, LANES)
    nrows = cdiv(nhi * ncls, 8) * 8
    rows = cdiv(fhi * fcls + nrows, 16) * 16
    near_at = cdiv(far, 64) * 64
    slots = cdiv(near_at + near, LANES) * LANES
    dims = (targets, far, near, fcls, ncls, fhi, nhi, rows, slots, near_at, nrows)

    def like(x):
        return jax.ShapeDtypeStruct(x.shape, BF16)

    vmem = pl.BlockSpec(memory_space=pltpu.VMEM)
    smem = pl.BlockSpec(memory_space=pltpu.SMEM)
    parts = pl.pallas_call(
        functools.partial(counts_kernel, dims),
        out_shape=(
            jax.ShapeDtypeStruct((targets * fcls, fhi * LANES), BF16),
            jax.ShapeDtypeStruct((targets * nrows, LANES), F32),
            like(far_ops), like(far_ops), like(near_ops), like(near_ops),
            like(local_to_target), like(local_to_target),
        ),
        in_specs=[smem] + [vmem] * 7,
        out_specs=(vmem,) * 8,
        scratch_shapes=[pltpu.VMEM((targets, slots), jnp.int32), pltpu.VMEM((targets, slots), jnp.int32)],
        name="counts",
    )(far_count, far_src, far_kind, near_src, near_kind, far_ops, near_ops, local_to_target)
    return pl.pallas_call(
        functools.partial(field_kernel, dims),
        out_shape=jax.ShapeDtypeStruct((targets, width_q), F32),
        in_specs=[vmem] * 12,
        out_specs=vmem,
        scratch_shapes=[pltpu.VMEM((cdiv(width_p, LANES), targets * fcls, LANES), F32)],
        name="field",
    )(*parts, range_multi, ghost_multi, chebyshev, ghost_cheb)


def solution(mesh):
    both = P(("morton", "grp"), None)
    in_specs = (both, both, P("morton", None), both, both, P(("morton", "grp")), both, both, P(), P(), P())
    return jax.shard_map(shards, mesh=mesh, in_specs=in_specs, out_specs=both, check_vma=False)
```

```python
import functools

import jax
import jax.numpy as jnp
from jax import lax
from jax.experimental import pallas as pl
from jax.experimental.pallas import tpu as pltpu
from jax.sharding import PartitionSpec as P

NCAP = 16
LANES = 128
SUB = 8
F32 = jnp.float32
BF16 = jnp.bfloat16
VMEM = pl.BlockSpec(memory_space=pltpu.VMEM)
SMEM = pl.BlockSpec(memory_space=pltpu.SMEM)
HBM = pl.BlockSpec(memory_space=pltpu.HBM)


def cdiv(a, b):
    return -(-a // b)


def log2(n):
    assert n & (n - 1) == 0, n
    return n.bit_length() - 1


def split(x):
    hi = x.astype(BF16)
    return hi, (x - hi.astype(F32)).astype(BF16)


def mm(a, b):
    return lax.dot_general(a, b, (((1,), (0,)), ((), ())), preferred_element_type=F32)


def dot3(x, w):
    wh, wl = split(w)
    xh, xl = split(x)
    both = mm(jnp.concatenate([xh, xl], axis=0), wh)
    n = x.shape[0]
    return both[:n] + both[n:] + mm(xh, wl)


class Plan:
    def __init__(self, multi, cheb, ghost_rows, far_src, near_src, far_ops, near_ops, groups):
        self.targets, self.p = multi.shape
        self.q = cheb.shape[1]
        self.members, self.cap = ghost_rows.shape
        self.ncap = NCAP
        self.far, self.near = far_src.shape[1], near_src.shape[1]
        self.fcls, self.ncls = far_ops.shape[0], near_ops.shape[0]
        self.range = self.targets * groups
        self.halves = 2 if groups % 2 == 0 else 1
        self.fc, self.nc = self.cap // self.halves, self.ncap // self.halves
        self.ftable = self.range + self.members * self.cap
        self.ntable = self.targets + self.members * self.ncap
        self.fhi, self.nhi = cdiv(self.ftable, LANES), cdiv(self.ntable, LANES)
        self.nrows = cdiv(self.nhi * self.ncls, SUB) * SUB
        self.rows = cdiv(self.fhi * self.fcls + self.nrows, 16) * 16
        self.near_at = cdiv(self.far, 64) * 64
        self.slots = cdiv(self.near_at + self.near, LANES) * LANES
        self.pf, self.pt = divmod(self.p, LANES)
        self.width = self.p + self.q
        self.qf = cdiv(self.width, LANES) - self.pf
        self.step = 1 << (self.pt - 1).bit_length()
        self.per = LANES // self.step
        self.tail_rows = self.fc // self.per
        self.at_tail = self.pf * self.fc
        self.at_cheb = self.at_tail + self.tail_rows
        self.block = self.at_cheb + self.qf * self.nc
        assert self.tail_rows % SUB == 0 and self.nc % SUB == 0


def pack_kernel(d, par_ref, ghost_ref, table_ref, send_ref, tail_ref):
    par = par_ref[0]
    lane = lax.broadcasted_iota(jnp.int32, (d.tail_rows, LANES), 1)
    first = d.pf * LANES

    def body(r, carry):
        for c in range(d.fc):
            row = table_ref[pl.ds(ghost_ref[r, par * d.fc + c], 1), :]
            for j in range(d.pf):
                send_ref[r, j * d.fc + c:j * d.fc + c + 1, :] = row[:, j * LANES:(j + 1) * LANES]
            tail_ref[c:c + 1, :] = row[:, first:first + LANES]
        merged = jnp.zeros((d.tail_rows, LANES), F32)
        for g in range(d.per):
            part = pltpu.roll(tail_ref[g * d.tail_rows:(g + 1) * d.tail_rows, :], (g * d.step) % LANES, 1)
            merged = jnp.where((lane >= g * d.step) & (lane < g * d.step + d.pt), part, merged)
        send_ref[r, d.at_tail:d.at_cheb, :] = merged
        for c in range(d.nc):
            row = table_ref[pl.ds(ghost_ref[r, par * d.nc + c], 1), :]
            for j in range(d.qf):
                at = (d.pf + j) * LANES
                n = min(LANES, d.width - at)
                send_ref[r, d.at_cheb + j * d.nc + c:d.at_cheb + j * d.nc + c + 1, :n] = row[:, at:at + n]
        return carry

    lax.fori_loop(0, d.members, body, 0)


def counts_kernel(d, par_ref, cnt_ref, fsrc_ref, fkind_ref, nsrc_ref, nkind_ref, wf_ref, wn_ref, c_ref, lo_ref):
    group = 4
    par = par_ref[0]

    def place(src, own, cap, part):
        n = src - own
        c = n & (cap - 1)
        half = (c >> log2(part)) ^ par if d.halves == 2 else 0
        ghost = own + half * (d.members * part) + (n >> log2(cap)) * part + (c & (part - 1))
        return jnp.where(n < 0, src, ghost)

    fsrc = place(fsrc_ref[...], d.range, d.cap, d.fc)
    nsrc = place(nsrc_ref[...], d.targets, d.ncap, d.nc)
    c_ref[...] = jnp.full(c_ref.shape, -1, jnp.int32)
    lo_ref[...] = jnp.zeros(lo_ref.shape, jnp.int32)
    c_ref[:, :d.far] = (fsrc >> 7) * d.fcls + fkind_ref[...]
    lo_ref[:, :d.far] = fsrc & (LANES - 1)
    c_ref[:, d.near_at:d.near_at + d.near] = d.fhi * d.fcls + (nsrc >> 7) * d.ncls + nkind_ref[...]
    lo_ref[:, d.near_at:d.near_at + d.near] = nsrc & (LANES - 1)
    lane = lax.broadcasted_iota(jnp.int32, (1, d.slots), 1)
    row_id = lax.broadcasted_iota(jnp.int32, (d.rows, d.slots), 0)
    lo_id = lax.broadcasted_iota(jnp.int32, (LANES, d.slots), 0)

    def body(step, carry):
        for i in range(group):
            t = step * group + i
            live = (lane < cnt_ref[t]) | (lane >= d.near_at)
            c_row = jnp.where(live, c_ref[pl.ds(t, 1), :], -1)
            one_c = jnp.where(row_id == c_row, 1.0, 0.0).astype(BF16)
            one_lo = jnp.where(lo_id == lo_ref[pl.ds(t, 1), :], 1.0, 0.0).astype(BF16)
            w = lax.dot_general(one_c, one_lo, (((1,), (1,)), ((), ())), preferred_element_type=F32)
            at = pl.multiple_of(t * d.fcls, d.fcls)
            for h in range(d.fhi):
                wf_ref[pl.ds(at, d.fcls), h * LANES:(h + 1) * LANES] = w[h * d.fcls:(h + 1) * d.fcls].astype(BF16)
            wn_ref[pl.ds(pl.multiple_of(t * d.nrows, d.nrows), d.nrows), :] = (
                w[d.fhi * d.fcls:d.fhi * d.fcls + d.nrows])
        return carry

    lax.fori_loop(0, d.targets // group, body, 0)


def field_kernel(d, *refs):
    hbm, out_ref, vm, fs_ref, sem = refs[:9], refs[9], refs[10:19], refs[19], refs[20]
    copies = [pltpu.make_async_copy(hbm[i], vm[i], sem.at[i]) for i in range(9)]
    for copy in copies:
        copy.start()
    wf_ref, own_ref, pair_ref, multi_ref, wn_ref, cheb_ref, fops_ref, l2t_ref, nops_ref = vm
    got = (own_ref, pair_ref)[:d.halves]
    for i in range(4):
        copies[i].wait()
    far_sum = jnp.zeros((d.targets * d.fcls, d.p), F32)
    at = 0
    for part in (multi_ref,) + got:
        if part is multi_ref:
            rows = part[:, :d.p]
        else:
            cut = [part[:, j * d.fc:(j + 1) * d.fc, :].reshape(-1, LANES) for j in range(d.pf)]
            tail = part[:, d.at_tail:d.at_cheb, :].reshape(-1, LANES)
            tails = [pltpu.roll(tail, (-g * d.step) % LANES, 1).reshape(d.members, d.tail_rows, LANES)
                     for g in range(d.per)]
            tails = jnp.concatenate(tails, axis=1).reshape(-1, LANES)[:, :d.pt]
            rows = jnp.concatenate(cut + [tails], axis=1)
        rh, rl = split(rows)
        w = wf_ref[:, at:at + rows.shape[0]]
        far_sum += mm(w, rh) + mm(w, rl)
        at += rows.shape[0]
    cuts = [(at, min(at + LANES, d.p)) for at in range(0, d.p, LANES)]
    for i, (first, last) in enumerate(cuts):
        fs_ref[i, :, :last - first] = far_sum[:, first:last]
    copies[6].wait()
    local = jnp.zeros((d.targets, d.p), F32)
    for k in range(d.fcls):
        x = [fs_ref[i, pl.ds(k, d.targets, stride=d.fcls), :][:, :last - first] for i, (first, last) in enumerate(cuts)]
        local += dot3(jnp.concatenate(x, axis=1), fops_ref[k])
    for i in (4, 5):
        copies[i].wait()
    tables = [cheb_ref[...]]
    for part in got:
        cut = [part[:, d.at_cheb + j * d.nc:d.at_cheb + (j + 1) * d.nc, :].reshape(-1, LANES) for j in range(d.qf)]
        tables.append(jnp.concatenate(cut, axis=1)[:, d.pt:d.pt + d.q])
    th, tl = split(jnp.concatenate(tables, axis=0))
    sums = jnp.zeros((d.ncls * d.targets, d.q), F32)
    for h in range(d.nhi):
        first, last = h * LANES, min((h + 1) * LANES, d.ntable)
        w = jnp.concatenate(
            [wn_ref[pl.ds(h * d.ncls + k, d.targets, stride=d.nrows), :] for k in range(d.ncls)], axis=0
        ).astype(BF16)[:, :last - first]
        sums += mm(w, th[first:last]) + mm(w, tl[first:last])
    copies[7].wait()
    acc = dot3(local, l2t_ref[...])
    copies[8].wait()
    for k in range(d.ncls):
        acc += dot3(sums[k * d.targets:(k + 1) * d.targets], nops_ref[k])
    out_ref[...] = acc


def shards(groups, multipoles, chebyshev, ghost_rows, far_src, far_kind, far_count, near_src, near_kind,
           far_ops, near_ops, local_to_target):
    d = Plan(multipoles, chebyshev, ghost_rows, far_src, near_src, far_ops, near_ops, groups)
    packed = jnp.concatenate([multipoles, chebyshev], axis=1)
    table = lax.all_gather(packed, "grp", axis=0, tiled=True)
    parity = (lax.axis_index("grp") & 1).astype(jnp.int32).reshape(1)
    send = pl.pallas_call(
        functools.partial(pack_kernel, d),
        out_shape=jax.ShapeDtypeStruct((d.members, d.block, LANES), F32),
        in_specs=[SMEM, SMEM, VMEM],
        out_specs=VMEM,
        scratch_shapes=[pltpu.VMEM((d.fc, LANES), F32)],
        compiler_params=pltpu.CompilerParams(vmem_limit_bytes=16 << 20),
        name="pack",
    )(parity, ghost_rows, table)
    got = lax.all_to_all(send, "morton", split_axis=0, concat_axis=0, tiled=True)
    wf, wn = pl.pallas_call(
        functools.partial(counts_kernel, d),
        out_shape=(
            jax.ShapeDtypeStruct((d.targets * d.fcls, d.fhi * LANES), BF16),
            jax.ShapeDtypeStruct((d.targets * d.nrows, LANES), F32),
        ),
        in_specs=[SMEM, SMEM] + [VMEM] * 4,
        out_specs=(VMEM,) * 2,
        scratch_shapes=[pltpu.VMEM((d.targets, d.slots), jnp.int32)] * 2,
        cost_estimate=pl.CostEstimate(flops=20_000_000_000, transcendentals=0, bytes_accessed=2 << 20),
        name="counts",
    )(parity, far_count, far_src, far_kind, near_src, near_kind)
    got, wf, wn = lax.optimization_barrier((got, wf, wn))
    if d.halves == 2:
        pair = lax.ppermute(got, "grp", [(i, i ^ 1) for i in range(groups)])
    else:
        pair = got
    inputs = (wf, got, pair, table, wn, chebyshev, far_ops, local_to_target, near_ops)
    return pl.pallas_call(
        functools.partial(field_kernel, d),
        out_shape=jax.ShapeDtypeStruct((d.targets, d.q), F32),
        in_specs=[HBM] * 9,
        out_specs=VMEM,
        scratch_shapes=[pltpu.VMEM(x.shape, x.dtype) for x in inputs]
        + [pltpu.VMEM((cdiv(d.p, LANES), d.targets * d.fcls, LANES), F32), pltpu.SemaphoreType.DMA((9,))],
        name="field",
    )(*inputs)


def solution(mesh):
    both = P(("morton", "grp"), None)
    in_specs = (both, both, P("morton", None), both, both, P(("morton", "grp")), both, both, P(), P(), P())
    return jax.shard_map(functools.partial(shards, mesh.shape["grp"]), mesh=mesh, in_specs=in_specs,
                         out_specs=both, check_vma=False)
```

```python
import functools

import jax
import jax.numpy as jnp
from jax import lax
from jax.experimental import pallas as pl
from jax.experimental.pallas import tpu as pltpu
from jax.sharding import PartitionSpec as P

NCAP = 16
LANES = 128
SUB = 8
PACK = 16
F32 = jnp.float32
BF16 = jnp.bfloat16
I32 = jnp.int32
VMEM = pl.BlockSpec(memory_space=pltpu.VMEM)
SMEM = pl.BlockSpec(memory_space=pltpu.SMEM)
HBM = pl.BlockSpec(memory_space=pltpu.HBM)


def cdiv(a, b):
    return -(-a // b)


def up(a, b):
    return cdiv(a, b) * b


def log2(n):
    assert n & (n - 1) == 0, n
    return n.bit_length() - 1


def split(x):
    hi = x.astype(BF16)
    return hi, (x - hi.astype(F32)).astype(BF16)


def mm(a, b):
    return lax.dot_general(a, b, (((1,), (0,)), ((), ())), preferred_element_type=F32)


def dot3(x, wh, wl):
    xh, xl = split(x)
    both = mm(jnp.concatenate([xh, xl], axis=0), wh)
    n = x.shape[0]
    return both[:n] + both[n:] + mm(xh, wl)


class Plan:
    def __init__(self, multi, cheb, ghost_rows, far_src, near_src, far_ops, near_ops, groups):
        self.targets, self.p = multi.shape
        self.q = cheb.shape[1]
        self.members, self.cap = ghost_rows.shape
        self.ncap = NCAP
        self.far, self.near = far_src.shape[1], near_src.shape[1]
        self.fcls, self.ncls = far_ops.shape[0], near_ops.shape[0]
        self.range = self.targets * groups
        self.flipped = groups & (groups - 1) == 0
        self.halves = 2 if groups % 2 == 0 else 1
        self.fc, self.nc = self.cap // self.halves, self.ncap // self.halves
        self.ghosts = self.members * self.cap
        self.far_off = self.members // 2
        assert self.members % 2 == 0
        self.ftable = self.range + self.ghosts
        self.ntable = self.targets + self.members * self.ncap
        assert self.range % LANES == 0 and self.ghosts % LANES == 0
        self.fhi, self.nhi = self.ftable // LANES, cdiv(self.ntable, LANES)
        self.nrows = up(self.nhi * self.ncls, SUB)
        self.rows = up(self.fhi * self.fcls + self.nrows, PACK)
        self.near_at = up(self.far, 64)
        self.slots = up(self.near_at + self.near, LANES)
        self.qpad = up(self.q, LANES)
        self.pf, self.pt = divmod(self.p, LANES)
        self.width = self.p + self.q
        self.qf = cdiv(self.width, LANES) - self.pf
        self.step = 1 << (self.pt - 1).bit_length()
        self.per = LANES // self.step
        self.tail_rows = self.fc // self.per
        self.at_tail = self.pf * self.fc
        self.at_cheb = self.at_tail + self.tail_rows
        self.block = self.at_cheb + self.qf * self.nc
        assert self.tail_rows % SUB == 0 and self.nc % SUB == 0
        self.cuts = [(at, min(at + LANES, self.p)) for at in range(0, self.p, LANES)]


def whereabouts(d):
    helper, member = lax.axis_index("grp").astype(I32), lax.axis_index("morton").astype(I32)
    return helper & 1, helper * d.targets if d.flipped else 0, member >> 1, member & 1


def fetch(sources, targets, sem):
    copies = [pltpu.make_async_copy(x, y, sem.at[i]) for i, (x, y) in enumerate(zip(sources, targets))]
    for copy in copies:
        copy.start()
    return copies


def join_kernel(multi, cheb, out_ref, multi_ref, cheb_ref, sem):
    for copy in fetch((multi, cheb), (multi_ref, cheb_ref), sem):
        copy.wait()
    out_ref[...] = jnp.concatenate([multi_ref[...], cheb_ref[...]], axis=1)


def pairs_kernel(d, keep_ref, swap_ref, *outs):
    for i, out in enumerate(outs):
        out[0] = keep_ref[i]
        out[1] = swap_ref[i]


def pack_kernel(d, ghost_ref, *refs):
    parts, outs = refs[:-2], refs[-2:]
    par, flip, high, low = whereabouts(d)
    ids = ghost_ref[...] ^ flip
    first = [ids[:, :d.fc], ids[:, :d.nc]]
    if d.halves == 2:
        first = [jnp.where(par == 0, first[0], ids[:, d.fc:2 * d.fc]),
                 jnp.where(par == 0, first[1], ids[:, d.nc:2 * d.nc])]
    ids = jnp.concatenate(first + [jnp.zeros((d.members, LANES - d.fc - d.nc), I32)], axis=1)
    ids = pltpu.roll(ids, (d.members - 2 * high) % d.members, 0)
    even = (lax.broadcasted_iota(I32, ids.shape, 0) & 1) == 0
    swapped = jnp.where(even, pltpu.roll(ids, d.members - 1, 0), pltpu.roll(ids, 1, 0))
    columns = jnp.where(low == 0, ids, swapped).T
    lane = lax.broadcasted_iota(I32, (d.fc, d.range), 1)

    def pick(at, n):
        hot = [jnp.where(columns[at:at + n, r:r + 1] == lane[:n], 1.0, 0.0) for r in range(d.members)]
        return jnp.concatenate(hot, axis=0).astype(BF16)

    def put(first, rows, lanes, value):
        value = value.reshape(d.far_off, 2, rows, lanes)
        for i in range(2):
            outs[i][:, first:first + rows, :lanes] = value[:, i]

    hi, lo = split(jnp.concatenate([part[...] for part in parts], axis=0))
    far_hot, near_hot = pick(0, d.fc), pick(d.fc, d.nc)
    far = mm(far_hot, hi[:, :d.p]) + mm(far_hot, lo[:, :d.p])
    for j in range(d.pf):
        put(j * d.fc, d.fc, LANES, far[:, j * LANES:(j + 1) * LANES])
    tail = jnp.concatenate([far[:, d.pf * LANES:], jnp.zeros((far.shape[0], LANES - d.pt), F32)], axis=1)
    tail = tail.reshape(d.members, d.fc, LANES)
    merged = tail[:, :d.tail_rows].reshape(-1, LANES)
    for g in range(1, d.per):
        part = tail[:, g * d.tail_rows:(g + 1) * d.tail_rows].reshape(-1, LANES)
        merged = merged + pltpu.roll(part, g * d.step, 1)
    put(d.at_tail, d.tail_rows, LANES, merged)
    start = d.pf * LANES
    near = mm(near_hot, hi[:, start:]) + mm(near_hot, lo[:, start:])
    for j in range(d.qf):
        n = min(LANES, d.width - start - j * LANES)
        put(d.at_cheb + j * d.nc, d.nc, n, near[:, j * LANES:j * LANES + n])


def store_sums(d, fs_ref, far_sum, at=0):
    for i, (first, last) in enumerate(d.cuts):
        fs_ref[i, at:at + far_sum.shape[0], :last - first] = far_sum[:, first:last]


def load_sums(d, fs_ref, k):
    x = [fs_ref[i, pl.ds(k, d.targets, stride=d.fcls), :][:, :last - first] for i, (first, last) in enumerate(d.cuts)]
    return jnp.concatenate(x, axis=1)


def contract(d, fs_ref, tmp_ref, local, fh, fl):
    chains = [None, None]
    for k in range(d.fcls):
        part = dot3(load_sums(d, fs_ref, k), fh[k], fl[k])
        chains[k % 2] = part if chains[k % 2] is None else chains[k % 2] + part
    if chains[1] is None:
        return local + chains[0]
    tmp_ref[...] = chains[1]
    return local + chains[0] + tmp_ref[...]


def operators_kernel(d, fops_ref, l2t_ref, nops_ref, fh, fl, lh, ll, nh, nl):
    for k in range(d.ncls):
        nh[k, :d.q], nl[k, :d.q] = split(nops_ref[k])
        if d.qpad > d.q:
            nh[k, d.q:] = jnp.zeros((d.qpad - d.q, d.q), BF16)
            nl[k, d.q:] = jnp.zeros((d.qpad - d.q, d.q), BF16)
    for k in range(d.fcls):
        fh[k], fl[k] = split(fops_ref[k])
    lh[...], ll[...] = split(l2t_ref[...])


def counts_kernel(d, *refs):
    lists, (wf_ref, wn_ref, c_ref, lo_ref), local, sem = refs[:5], refs[5:9], refs[9:14], refs[14]
    copies = fetch(lists, local, sem)
    cnt_ref, fsrc_ref, fkind_ref, nsrc_ref, nkind_ref = local
    for copy in copies:
        copy.wait()
    group = 4
    par, flip, high, low = whereabouts(d)

    def turn(x):
        tall = up(d.near, SUB) - d.near
        x = jnp.concatenate([x, jnp.zeros((tall, d.targets), I32)], axis=0) if tall else x
        wide = up(d.targets, LANES) - d.targets
        x = jnp.concatenate([x, jnp.zeros((x.shape[0], wide), I32)], axis=1) if wide else x
        return x.T[:d.targets, :d.near]

    def place(src, own, cap, part):
        n = src - own
        c = n & (cap - 1)
        owner = n >> log2(cap)
        away = high - (owner >> 1)
        away = jnp.where(away < 0, away + d.far_off, away)
        half = (c >> log2(part)) ^ par if d.halves == 2 else 0
        block = half * d.members + away * 2 + ((owner & 1) ^ low)
        return own + block * part + (c & (part - 1))

    fsrc, nsrc, nkind = fsrc_ref[...], turn(nsrc_ref[...]), turn(nkind_ref[...])
    fsrc = jnp.where(fsrc < d.range, fsrc ^ flip, place(fsrc, d.range, d.cap, d.fc))
    nsrc = jnp.where(nsrc < d.targets, nsrc, place(nsrc, d.targets, d.ncap, d.nc))
    c_ref[...] = jnp.full(c_ref.shape, -1, I32)
    lo_ref[...] = jnp.zeros(lo_ref.shape, I32)
    c_ref[:, :d.far] = (fsrc >> 7) * d.fcls + fkind_ref[...]
    lo_ref[:, :d.far] = fsrc & (LANES - 1)
    c_ref[:, d.near_at:d.near_at + d.near] = d.fhi * d.fcls + (nsrc >> 7) * d.ncls + nkind
    lo_ref[:, d.near_at:d.near_at + d.near] = nsrc & (LANES - 1)
    lane = lax.broadcasted_iota(I32, (1, d.slots), 1)
    row_id = lax.broadcasted_iota(I32, (d.rows, d.slots), 0)
    lo_id = lax.broadcasted_iota(I32, (LANES, d.slots), 0)

    def body(step, carry):
        for i in range(group):
            t = step * group + i
            live = (lane < cnt_ref[t]) | (lane >= d.near_at)
            c_row = jnp.where(live, c_ref[pl.ds(t, 1), :], -1)
            one_c = jnp.where(row_id == c_row, 1.0, 0.0).astype(BF16)
            one_lo = jnp.where(lo_id == lo_ref[pl.ds(t, 1), :], 1.0, 0.0).astype(BF16)
            w = lax.dot_general(one_c, one_lo, (((1,), (1,)), ((), ())), preferred_element_type=F32)
            at = pl.multiple_of(t * d.fcls, d.fcls)
            for h in range(d.fhi):
                wf_ref[pl.ds(at, d.fcls), h * LANES:(h + 1) * LANES] = w[h * d.fcls:(h + 1) * d.fcls].astype(BF16)
            wn_ref[pl.ds(pl.multiple_of(t * d.nrows, d.nrows), d.nrows), :] = (
                w[d.fhi * d.fcls:d.fhi * d.fcls + d.nrows])
        return carry

    lax.fori_loop(0, d.targets // group, body, 0)


def far_sums(d, fs_ref, w_ref, first, hi, lo):
    size = d.targets * d.fcls // 2
    for i in range(2):
        w = w_ref[i * size:(i + 1) * size, first:first + hi.shape[0]]
        store_sums(d, fs_ref, mm(w, hi) + mm(w, lo), i * size)


def own_kernel(d, wf_ref, fh, fl, *refs):
    parts, (local_ref, fs_ref, tmp_ref) = refs[:-3], refs[-3:]
    hi, lo = split(jnp.concatenate([part[:, :d.p] for part in parts], axis=0))
    far_sums(d, fs_ref, wf_ref, 0, hi, lo)
    local_ref[...] = contract(d, fs_ref, tmp_ref, jnp.zeros((d.targets, d.p), F32), fh, fl)


def field_kernel(d, *refs):
    n = d.far_off * d.halves
    got, refs = refs[:n], refs[n:]
    wf_ref, wn_ref, local_ref, cheb_ref, fh, fl, lh, ll, nh, nl, out_ref, fs_ref, tmp_ref = refs
    rows, tables = [], [cheb_ref[...]]
    for part in got:
        cut = [part[:, j * d.fc:(j + 1) * d.fc, :].reshape(-1, LANES) for j in range(d.pf)]
        tail = part[:, d.at_tail:d.at_cheb, :].reshape(-1, LANES)
        tails = [tail if g == 0 else pltpu.roll(tail, (-g * d.step) % LANES, 1) for g in range(d.per)]
        tails = jnp.concatenate([t.reshape(2, d.tail_rows, LANES) for t in tails], axis=1)
        rows.append(jnp.concatenate(cut + [tails.reshape(-1, LANES)[:, :d.pt]], axis=1))
        t = part[:, d.at_cheb:, :]
        tables.append(jnp.concatenate(
            [t[:, j * d.nc:(j + 1) * d.nc, :].reshape(-1, LANES) for j in range(d.qf)], axis=1)[:, d.pt:d.pt + d.q])
    hi, lo = split(jnp.concatenate(rows, axis=0))
    far_sums(d, fs_ref, wf_ref, d.range, hi, lo)
    table = jnp.concatenate(tables, axis=0)
    if d.qpad > d.q:
        table = jnp.concatenate([table, jnp.zeros((d.ntable, d.qpad - d.q), F32)], axis=1)
    th, tl = split(table)
    w = jnp.concatenate([
        jnp.concatenate([wn_ref[pl.ds(h * d.ncls + k, d.targets, stride=d.nrows), :] for k in range(d.ncls)], axis=0)
        for h in range(d.nhi)], axis=1).astype(BF16)[:, :d.ntable]
    sums = mm(w, th) + mm(w, tl)
    x = jnp.concatenate([sums[k * d.targets:(k + 1) * d.targets] for k in range(d.ncls)], axis=1)
    acc = dot3(x, nh[...].reshape(d.ncls * d.qpad, d.q), nl[...].reshape(d.ncls * d.qpad, d.q))
    local = contract(d, fs_ref, tmp_ref, local_ref[...], fh, fl)
    out_ref[...] = acc + dot3(local, lh[...], ll[...])


def gather_group(x, groups, beside):
    if groups & (groups - 1) or groups == 1:
        return [lax.all_gather(x, "grp", axis=0, tiled=True)], beside
    blocks = {0: x}
    for bit in reversed(range(log2(groups))):
        flip = 1 << bit
        pairs = [(i, i ^ flip) for i in range(groups)]
        blocks |= {i | flip: lax.ppermute(block, "grp", pairs) for i, block in blocks.items()}
        if flip == groups // 2:
            blocks[flip], *beside = lax.optimization_barrier((blocks[flip], *beside))
    return [blocks[i] for i in range(groups)], beside


def like(x, dtype=BF16):
    return jax.ShapeDtypeStruct(x.shape, dtype)


def pinned(*xs):
    return [pltpu.with_memory_space_constraint(x, pltpu.HBM) for x in xs]


def limit(mib, flops=10_000_000_000):
    return dict(compiler_params=pltpu.CompilerParams(vmem_limit_bytes=mib << 20),
                cost_estimate=pl.CostEstimate(flops=flops, transcendentals=0, bytes_accessed=2 << 20))


def exchange(d, groups, keep, send, beside):
    partner = [(i, i ^ 1) for i in range(d.members)]
    swapped = lax.ppermute(send, "morton", partner)
    swapped, *beside = lax.optimization_barrier((swapped, *beside))
    pieces = list(pl.pallas_call(
        functools.partial(pairs_kernel, d),
        out_shape=(jax.ShapeDtypeStruct((2, d.block, LANES), F32),) * d.far_off,
        in_specs=[VMEM] * 2,
        out_specs=(VMEM,) * d.far_off,
        name="pairs",
        **limit(24, 1_000_000),
    )(keep, swapped))
    for away in range(1, d.far_off):
        shift = [(i, (i + 2 * away) % d.members) for i in range(d.members)]
        pieces[away] = lax.ppermute(pieces[away], "morton", shift)
    if d.halves == 2:
        pieces += [lax.ppermute(piece, "grp", [(i, i ^ 1) for i in range(groups)]) for piece in pieces]
    return pieces, beside


def shards(groups, multipoles, chebyshev, ghost_rows, far_src, far_kind, far_count, near_src, near_kind,
           far_ops, near_ops, local_to_target):
    d = Plan(multipoles, chebyshev, ghost_rows, far_src, near_src, far_ops, near_ops, groups)
    packed = pl.pallas_call(
        join_kernel,
        out_shape=jax.ShapeDtypeStruct((d.targets, d.width), F32),
        in_specs=[HBM] * 2,
        out_specs=VMEM,
        scratch_shapes=[pltpu.VMEM(multipoles.shape, F32), pltpu.VMEM(chebyshev.shape, F32),
                        pltpu.SemaphoreType.DMA((2,))],
        name="join",
        **limit(24, 1_000_000),
    )(*pinned(multipoles, chebyshev))

    padded = jax.ShapeDtypeStruct((d.ncls, d.qpad, d.q), BF16)
    ops = (far_ops, local_to_target, near_ops)
    sums = pltpu.VMEM((len(d.cuts), d.targets * d.fcls, LANES), F32)
    part_sum = pltpu.VMEM((d.targets, d.p), F32)
    cuts = pl.pallas_call(
        functools.partial(operators_kernel, d),
        out_shape=(like(far_ops), like(far_ops), like(local_to_target), like(local_to_target), padded, padded),
        in_specs=[VMEM] * 3,
        out_specs=(VMEM,) * 6,
        name="operators",
        **limit(24),
    )(*ops)
    lists = (far_count, far_src, far_kind, near_src.T, near_kind.T)
    wf, wn = pl.pallas_call(
        functools.partial(counts_kernel, d),
        out_shape=(jax.ShapeDtypeStruct((d.targets * d.fcls, d.ftable), BF16),
                   jax.ShapeDtypeStruct((d.targets * d.nrows, LANES), F32)),
        in_specs=[HBM] * 5,
        out_specs=(VMEM,) * 2,
        scratch_shapes=[pltpu.VMEM((d.targets, d.slots), I32)] * 2
        + [pltpu.SMEM(lists[0].shape, I32)] + [pltpu.VMEM(x.shape, I32) for x in lists[1:]]
        + [pltpu.SemaphoreType.DMA((5,))],
        name="counts",
        **limit(24),
    )(*pinned(*lists))
    parts, (wf, wn) = gather_group(packed, groups, (wf, wn))
    block = jax.ShapeDtypeStruct((d.far_off, d.block, LANES), F32)
    keep, send = pl.pallas_call(
        functools.partial(pack_kernel, d),
        out_shape=(block, block),
        in_specs=[VMEM] * (1 + len(parts)),
        out_specs=(VMEM,) * 2,
        name="pack",
        **limit(24, 1_000_000),
    )(ghost_rows, *parts)
    pieces, cuts = exchange(d, groups, keep, send, cuts)
    fh, fl = cuts[:2]
    local = pl.pallas_call(
        functools.partial(own_kernel, d),
        out_shape=like(multipoles, F32),
        in_specs=[VMEM] * (3 + len(parts)),
        out_specs=VMEM,
        scratch_shapes=[sums, part_sum],
        name="own",
        **limit(24),
    )(wf, fh, fl, *parts)
    return pl.pallas_call(
        functools.partial(field_kernel, d),
        out_shape=jax.ShapeDtypeStruct((d.targets, d.q), F32),
        in_specs=[VMEM] * (len(pieces) + 10),
        out_specs=VMEM,
        scratch_shapes=[sums, part_sum],
        name="field",
        **limit(24),
    )(*pieces, wf, wn, local, chebyshev, *cuts)


def solution(mesh):
    both = P(("morton", "grp"), None)
    in_specs = (both, both, P("morton", None), both, both, P(("morton", "grp")), both, both, P(), P(), P())
    return jax.shard_map(functools.partial(shards, mesh.shape["grp"]), mesh=mesh, in_specs=in_specs,
                         out_specs=both, check_vma=False)
```
